32 devices in a mesh: chan: 4 (over z), pulse: 4 (over x, core), range: 2 (over y).
Axes of the slice: x: 2, y: 2, z: 4, core: 2. Of those that a mesh axis runs over, the one named last changes fastest.
Arguments:
- signal: bfloat16 [2, 64, 32, 8192], P(None, 'chan', 'pulse', 'range'), may hold values from -6 to 6
- steering: bfloat16 [2, 32, 64], replicated, may hold values from -0.5 to 0.5
- spectrum: float32 [2, 8192], replicated, may hold values from -6 to 6
Outputs:
- detection: float32 [32, 32, 8192], P('chan', 'pulse', 'range')
The draws below stay inside these ranges and needn't reach their ends.
All inputs are finite; a program needn't handle non-finite values.
Results may differ from the reference program's by a relative error of at most 0.0087.
Values may be sent and summed in bfloat16 or wider, within the bound.
A program may use at most 64 MiB of HBM per device.

```python
import math
import jax
import jax.numpy as jnp
from jax import lax

CH = 64
BEAMS = 32
GUARD = 4
TRAIN = 16
PULSES = 32
RANGE = 8192


def block_levels(own_key, shape, pieces, low, top_value):
    loudness, own = 1.0, jax.random.fold_in(own_key, 6)
    for position, blocks in pieces:
        draws = jnp.exp(jax.random.uniform(jax.random.fold_in(own, position), (blocks,), jnp.float32, low / len(pieces), top_value / len(pieces)))
        loudness = loudness * jnp.repeat(draws, shape[position] // blocks).reshape([-1 if axis == position else 1 for axis in range(len(shape))])
    return loudness


def scatter_about(stream_key, extent, width, reach, split=(), held_as=jnp.bfloat16):
    entries = jax.random.normal(stream_key, extent, jnp.float32) * width
    if len(split) > 0:
        entries = block_levels(stream_key, extent, split, -0.22, 0.18) * entries
    return jnp.clip(entries, min=-reach, max=reach).astype(held_as)


def setup_inputs(seed: int = 0) -> dict:
    splits = jax.random.split(jax.random.key(seed), 4)
    return {
        "signal": scatter_about(splits[0], (2, CH, PULSES, RANGE), 1.0, 6.0, ((1, 4), (2, 4), (3, 2))),
        "steering": scatter_about(splits[1], (2, BEAMS, CH), (2 * CH) ** -0.5, 0.5),
        "spectrum": scatter_about(splits[2], (2, RANGE), 1.0, 6.0, (), jnp.float32),
    }


NOISE_FLOOR = 0.25

def doppler_tables(pulse_count):
    row_ids = lax.broadcasted_iota(jnp.int32, (pulse_count, pulse_count), 0)
    col_ids = lax.broadcasted_iota(jnp.int32, (pulse_count, pulse_count), 1)
    phase_angle = (row_ids * col_ids % pulse_count).astype(jnp.float32) * (2.0 * math.pi / pulse_count)
    norm_scale = 1.0 / math.sqrt(pulse_count)
    table_real = (jnp.cos(phase_angle) * norm_scale).astype(jnp.bfloat16)
    table_imag = (-jnp.sin(phase_angle) * norm_scale).astype(jnp.bfloat16)
    return (table_real, table_imag)

def reference(signal, steering, spectrum):
    w_real = steering[0]
    w_imag = steering[1]
    stacked = jnp.concatenate([jnp.concatenate([w_real, -w_imag], 1), jnp.concatenate([w_imag, w_real], 1)], 0)
    flat_signal = signal.reshape(2 * CH, PULSES * RANGE)
    beam_data = jnp.dot(stacked, flat_signal, preferred_element_type=jnp.float32).astype(jnp.bfloat16)
    beam_data = beam_data.reshape(2, BEAMS, PULSES, RANGE)
    response = lax.complex(spectrum[0], spectrum[1])
    dop_real, dop_imag = doppler_tables(PULSES)
    halo_width = GUARD + TRAIN

    def one_beam(beam_slab):
        line_field = lax.complex(beam_slab[0].astype(jnp.float32), beam_slab[1].astype(jnp.float32))
        compressed = jnp.fft.ifft(jnp.fft.fft(line_field, axis=-1) * response, axis=-1)
        comp_real = jnp.real(compressed).astype(jnp.bfloat16)
        comp_imag = jnp.imag(compressed).astype(jnp.bfloat16)
        mixed_real = jnp.dot(dop_real, comp_real, preferred_element_type=jnp.float32) - jnp.dot(dop_imag, comp_imag, preferred_element_type=jnp.float32)
        mixed_imag = jnp.dot(dop_real, comp_imag, preferred_element_type=jnp.float32) + jnp.dot(dop_imag, comp_real, preferred_element_type=jnp.float32)
        power_map = mixed_real * mixed_real + mixed_imag * mixed_imag
        padded = jnp.pad(power_map, ((0, 0), (halo_width, halo_width)))
        window_sum = jnp.zeros_like(power_map)
        for offset in range(1, TRAIN + 1):
            left_start = halo_width - GUARD - offset
            right_start = halo_width + GUARD + offset
            window_sum = window_sum + padded[:, left_start:left_start + RANGE] + padded[:, right_start:right_start + RANGE]
        noise_level = window_sum / (2.0 * TRAIN)
        return power_map / (noise_level + NOISE_FLOOR)
    return lax.map(one_beam, jnp.transpose(beam_data, (1, 0, 2, 3)))
```

```python
import functools
import math

import jax
import jax.numpy as jnp
import numpy as np
from jax import lax
from jax.experimental import pallas as pl
from jax.experimental.pallas import tpu as pltpu
from jax.sharding import PartitionSpec as P

GUARD = 4
TRAIN = 16
NOISE_FLOOR = 0.25
LANES = 128
ROWS = 8
BF = jnp.bfloat16
F32 = jnp.float32
VM = 60 * 1024 * 1024


def dot(a, b):
    return jnp.dot(a, b, preferred_element_type=F32)


def doppler_table(count):
    ids = np.arange(count)
    angle = (np.outer(ids, ids) % count) * (2.0 * np.pi / count)
    scale = 1.0 / math.sqrt(count)
    return jnp.asarray(np.cos(angle) * scale, BF), jnp.asarray(-np.sin(angle) * scale, BF)


def expand(left_ids, left_tag, table, right_ids, right_tag):
    n, m = table.shape
    left = (jnp.asarray(left_ids, jnp.int32)[:, None] == jnp.arange(n)[None, :]).astype(BF)
    right = (jnp.arange(m)[:, None] == jnp.asarray(right_ids, jnp.int32)[None, :]).astype(BF)
    wide = dot(dot(left, table).astype(BF), right)
    same = jnp.asarray(left_tag, jnp.int32)[:, None] == jnp.asarray(right_tag, jnp.int32)[None, :]
    return jnp.where(same, wide, 0.0).astype(BF)


def grid_ids(*sizes):
    return [g.reshape(-1) for g in np.meshgrid(*[np.arange(s) for s in sizes], indexing="ij")]


def call(body, out_shape, name):
    return pl.pallas_call(
        body,
        out_shape=out_shape,
        compiler_params=pltpu.CompilerParams(vmem_limit_bytes=VM),
        name=name,
    )


def form_kernel(w_ref, x_ref, o_ref):
    o_ref[...] = dot(w_ref[...], x_ref[...]).astype(BF)


def range_kernel(blocks, x_ref, f_ref, fi_ref, t_ref, l_ref, li_ref, h_ref, o_ref):
    sources, rows, width = x_ref.shape
    per = width // LANES
    groups = rows // 16
    m_count = sources * per
    tile = []
    for g in range(groups):
        parts = [
            x_ref[s, 16 * g : 16 * g + 16, LANES * j : LANES * j + LANES]
            for s in range(sources)
            for j in range(per)
        ]
        tile.append(jnp.concatenate(parts, axis=0))
    outer = dot(f_ref[...], jnp.concatenate(tile, axis=1))
    tr, ti = t_ref[0], t_ref[1]
    hr, hi = h_ref[0], h_ref[1]
    back = []
    for g in range(groups):
        a = outer[:, LANES * g : LANES * g + LANES].reshape(m_count, 2, ROWS, LANES)
        ar, ai = a[:, 0], a[:, 1]
        b = jnp.concatenate([ar * tr - ai * ti, ar * ti + ai * tr], axis=-1)
        c = dot(b.reshape(m_count * ROWS, 2 * LANES).astype(BF), l_ref[...])
        c = c.reshape(m_count, ROWS, 2 * LANES)
        cr, ci = c[..., :LANES], c[..., LANES:]
        d = jnp.concatenate([cr * hr - ci * hi, cr * hi + ci * hr], axis=-1)
        e = dot(d.reshape(m_count * ROWS, 2 * LANES).astype(BF), li_ref[...])
        e = e.reshape(m_count, ROWS, 2 * LANES)
        er, ei = e[..., :LANES], e[..., LANES:]
        f = jnp.stack([er * tr + ei * ti, ei * tr - er * ti], axis=1)
        back.append(f.reshape(m_count * 16, LANES).astype(BF))
    y = dot(fi_ref[...], jnp.concatenate(back, axis=1)).astype(BF)
    span = m_count // blocks
    for d in range(blocks):
        for j in range(-1, span + 1):
            m = d * span + j
            for g in range(groups):
                if 0 <= m < m_count:
                    v = y[16 * m : 16 * m + 16, LANES * g : LANES * g + LANES]
                else:
                    v = jnp.zeros((16, LANES), BF)
                o_ref[d, 16 * g : 16 * g + 16, LANES * (j + 1) : LANES * (j + 2)] = v


def cfar_kernel(d_ref, x_ref, n_ref, o_ref):
    half = o_ref.shape[0]
    mix = dot(d_ref[...], x_ref[...])
    re, im = mix[:half], mix[half:]
    power = re * re + im * im
    narrow = power.astype(BF)
    for j in range(o_ref.shape[1] // LANES):
        noise = dot(narrow[:, LANES * j : LANES * (j + 3)], n_ref[...])
        own = power[:, LANES * (j + 1) : LANES * (j + 2)]
        o_ref[:, LANES * j : LANES * j + LANES] = (own / (noise + NOISE_FLOOR)).astype(BF)


def cfar_only_kernel(p_ref, n_ref, o_ref):
    narrow = p_ref[...].astype(BF)
    for j in range(o_ref.shape[1] // LANES):
        noise = dot(narrow[:, LANES * j : LANES * (j + 3)], n_ref[...])
        own = p_ref[:, LANES * (j + 1) : LANES * (j + 2)]
        o_ref[:, LANES * j : LANES * j + LANES] = (own / (noise + NOISE_FLOOR)).astype(BF)


def place_kernel(x_ref, o_ref):
    count, _, width = x_ref.shape
    for s in range(count):
        o_ref[:, width * s : width * s + width] = x_ref[s].astype(F32)


def complex_rows(re, im):
    top = np.stack([re, -im], -1)
    low = np.stack([im, re], -1)
    return np.stack([top, low], 1).reshape(2 * re.shape[0], 2 * re.shape[1])


def shards(signal, steering, spectrum):
    beams, chans = steering.shape[1], steering.shape[2]
    _, chan_own, pulse_own, gates = signal.shape
    zs, xs, ys = (lax.axis_size(a) for a in ("chan", "pulse", "range"))
    beam_own = beams // zs
    part = pulse_own // ys
    full = gates * ys
    block = gates // zs
    m_count = full // LANES
    groups = beam_own * part // ROWS
    pulses = pulse_own * xs

    w_real, w_imag = steering[0], steering[1]
    weights = jnp.concatenate(
        [jnp.concatenate([w_real, -w_imag], 1), jnp.concatenate([w_imag, w_real], 1)], 0
    )
    dy, dz, gr, cp, it = grid_ids(ys, zs, groups, 2, ROWS)
    bp = gr * ROWS + it
    left = cp * beams + dz * beam_own + bp // part
    left_pulse = dy * part + bp % part
    sz, ci, ch, pi = grid_ids(zs, 2, chan_own, pulse_own)
    right = ci * chans + sz * chan_own + ch
    form = expand(left, left_pulse, weights, right, pi)

    ms = np.arange(m_count)
    angle = 2.0 * np.pi * (np.outer(ms, ms) % m_count) / m_count
    outer_f = jnp.asarray(complex_rows(np.cos(angle), -np.sin(angle)), BF)
    outer_i = jnp.asarray(complex_rows(np.cos(angle), np.sin(angle)), BF)
    mk, mc, mi = grid_ids(m_count, 2, ROWS)
    outer_f = expand(mk * 2 + mc, mi, outer_f, mk * 2 + mc, mi)
    outer_i = expand(mk * 2 + mc, mi, outer_i, mk * 2 + mc, mi)
    ls = np.arange(LANES)
    angle = 2.0 * np.pi * (np.outer(ls, ls) % LANES) / LANES
    co, si = np.cos(angle), np.sin(angle)
    inner_f = jnp.asarray(np.block([[co, -si], [si, co]]), BF)
    inner_i = jnp.asarray(np.block([[co, si], [-si, co]]), BF)
    angle = 2.0 * np.pi * np.outer(ms, ls) / full
    twiddle = jnp.asarray(np.stack([np.cos(angle), -np.sin(angle)]), F32)
    spread = (2, m_count, ROWS, LANES)
    twiddle = jnp.broadcast_to(twiddle[:, :, None, :], spread)
    response = jnp.swapaxes(spectrum.reshape(2, LANES, m_count), 1, 2) * (1.0 / full)
    response = jnp.broadcast_to(response[:, :, None, :], spread)

    samples = lax.all_to_all(signal, "chan", split_axis=3, concat_axis=0, tiled=True)
    samples = samples.reshape(zs * 2 * chan_own * pulse_own, block)
    rows = 2 * beam_own * part
    formed = call(
        form_kernel, jax.ShapeDtypeStruct((ys * zs * rows, block), BF), "form"
    )(form, samples).reshape(ys * zs, rows, block)
    formed = lax.all_to_all(formed, ("range", "chan"), split_axis=0, concat_axis=0, tiled=True)

    blocks = ys * xs
    own = full // blocks
    padded = own + 2 * LANES
    packed = call(
        functools.partial(range_kernel, blocks),
        jax.ShapeDtypeStruct((blocks, rows, padded), BF),
        "compress",
    )(formed, outer_f, outer_i, twiddle, inner_f, inner_i, response)
    columns = lax.all_to_all(packed, ("range", "pulse"), split_axis=0, concat_axis=0, tiled=True)

    src, dst = np.arange(3 * LANES)[:, None] - LANES, np.arange(LANES)[None, :]
    gap = np.abs(src - dst)
    window = jnp.asarray(((gap > GUARD) & (gap <= GUARD + TRAIN)) / (2.0 * TRAIN), BF)

    dr, di = doppler_table(pulses)
    out_shape = jax.ShapeDtypeStruct((pulses * beam_own, own), BF)
    if 2 * pulses * beam_own <= 1024:
        table = jnp.concatenate([jnp.concatenate([dr, -di], 1), jnp.concatenate([di, dr], 1)], 0)
        oc, oq, ob, of = grid_ids(2, xs, beam_own, pulse_own)
        sy, sx, gr, cp, it = grid_ids(ys, xs, groups, 2, ROWS)
        bp = gr * ROWS + it
        pulse = sx * pulse_own + sy * part + bp % part
        mix = expand(oc * pulses + oq * pulse_own + of, ob, table, cp * pulses + pulse, bp // part)
        found = call(cfar_kernel, out_shape, "cfar")(
            mix, columns.reshape(blocks * rows, padded), window
        )
    else:
        v = columns.reshape(ys, xs, groups, 2, ROWS // part, part, padded)
        v = jnp.transpose(v, (3, 2, 4, 1, 0, 5, 6)).reshape(2, beam_own, pulses, padded)

        def product(t, x):
            return jnp.einsum("fp,bpr->fbr", t, x, preferred_element_type=F32)

        re = product(dr, v[0]) - product(di, v[1])
        im = product(dr, v[1]) + product(di, v[0])
        power = (re * re + im * im).reshape(xs, pulse_own, beam_own, padded)
        power = jnp.swapaxes(power, 1, 2).reshape(pulses * beam_own, padded)
        found = call(cfar_only_kernel, out_shape, "cfar")(power, window)
    found = found.reshape(xs, beam_own * pulse_own, own)
    found = lax.all_to_all(found, "pulse", split_axis=0, concat_axis=0, tiled=True)
    out = call(
        place_kernel, jax.ShapeDtypeStruct((beam_own * pulse_own, gates), F32), "place"
    )(found)
    return out.reshape(beam_own, pulse_own, gates)


def solution(mesh):
    in_specs = (P(None, "chan", "pulse", "range"), P(), P())
    out_specs = P("chan", "pulse", "range")
    return jax.shard_map(shards, mesh=mesh, in_specs=in_specs, out_specs=out_specs, check_vma=False)
```

```python
import functools
import math

import jax
import jax.numpy as jnp
import numpy as np
from jax import lax
from jax.experimental import pallas as pl
from jax.experimental.pallas import tpu as pltpu
from jax.sharding import PartitionSpec as P

GUARD = 4
TRAIN = 16
NOISE_FLOOR = 0.25
LANES = 128
ROWS = 8
BF = jnp.bfloat16
F32 = jnp.float32
VM = 60 * 1024 * 1024


def dot(a, b):
    return jnp.dot(a, b, preferred_element_type=F32)


def doppler_table(count):
    ids = np.arange(count)
    angle = (np.outer(ids, ids) % count) * (2.0 * np.pi / count)
    scale = 1.0 / math.sqrt(count)
    return jnp.asarray(np.cos(angle) * scale, BF), jnp.asarray(-np.sin(angle) * scale, BF)


def expand(left_ids, left_tag, table, right_ids, right_tag):
    n, m = table.shape
    left = (jnp.asarray(left_ids, jnp.int32)[:, None] == jnp.arange(n)[None, :]).astype(BF)
    right = (jnp.arange(m)[:, None] == jnp.asarray(right_ids, jnp.int32)[None, :]).astype(BF)
    wide = dot(dot(left, table).astype(BF), right)
    same = jnp.asarray(left_tag, jnp.int32)[:, None] == jnp.asarray(right_tag, jnp.int32)[None, :]
    return jnp.where(same, wide, 0.0).astype(BF)


def grid_ids(*sizes):
    return [g.reshape(-1) for g in np.meshgrid(*[np.arange(s) for s in sizes], indexing="ij")]


def call(body, out_shape, name):
    return pl.pallas_call(
        body,
        out_shape=out_shape,
        compiler_params=pltpu.CompilerParams(vmem_limit_bytes=VM),
        name=name,
    )


def form_kernel(w_ref, x_ref, o_ref):
    o_ref[...] = dot(w_ref[...], x_ref[...]).astype(BF)


def range_kernel(blocks, x_ref, f_ref, fi_ref, t_ref, l_ref, li_ref, h_ref, o_ref):
    sources, rows, width = x_ref.shape
    per = width // LANES
    groups = rows // 16
    m_count = sources * per
    tile = []
    for g in range(groups):
        parts = [
            x_ref[s, 16 * g : 16 * g + 16, LANES * j : LANES * j + LANES]
            for s in range(sources)
            for j in range(per)
        ]
        tile.append(jnp.concatenate(parts, axis=0))
    outer = dot(f_ref[...], jnp.concatenate(tile, axis=1))
    tr, ti = t_ref[0], t_ref[1]
    hr, hi = h_ref[0], h_ref[1]
    back = []
    for g in range(groups):
        a = outer[:, LANES * g : LANES * g + LANES].reshape(m_count, 2, ROWS, LANES)
        ar, ai = a[:, 0], a[:, 1]
        b = jnp.concatenate([ar * tr - ai * ti, ar * ti + ai * tr], axis=-1)
        c = dot(b.reshape(m_count * ROWS, 2 * LANES).astype(BF), l_ref[...])
        c = c.reshape(m_count, ROWS, 2 * LANES)
        cr, ci = c[..., :LANES], c[..., LANES:]
        d = jnp.concatenate([cr * hr - ci * hi, cr * hi + ci * hr], axis=-1)
        e = dot(d.reshape(m_count * ROWS, 2 * LANES).astype(BF), li_ref[...])
        e = e.reshape(m_count, ROWS, 2 * LANES)
        er, ei = e[..., :LANES], e[..., LANES:]
        f = jnp.stack([er * tr + ei * ti, ei * tr - er * ti], axis=1)
        back.append(f.reshape(m_count * 16, LANES).astype(BF))
    y = dot(fi_ref[...], jnp.concatenate(back, axis=1)).astype(BF)
    span = m_count // blocks
    for d in range(blocks):
        for j in range(-1, span + 1):
            m = d * span + j
            for g in range(groups):
                if 0 <= m < m_count:
                    v = y[16 * m : 16 * m + 16, LANES * g : LANES * g + LANES]
                else:
                    v = jnp.zeros((16, LANES), BF)
                o_ref[d, 16 * g : 16 * g + 16, LANES * (j + 1) : LANES * (j + 2)] = v


def cfar_kernel(d_ref, x_ref, n_ref, o_ref):
    half = d_ref.shape[0] // 2
    mix = dot(d_ref[...], x_ref[...].reshape(d_ref.shape[1], x_ref.shape[-1]))
    re, im = mix[:half], mix[half:]
    power = re * re + im * im
    narrow = power.astype(BF)
    shape = o_ref.shape[:-1] + (LANES,)
    for j in range(o_ref.shape[-1] // LANES):
        noise = dot(narrow[:, LANES * j : LANES * (j + 3)], n_ref[...])
        own = power[:, LANES * (j + 1) : LANES * (j + 2)]
        found = (own / (noise + NOISE_FLOOR)).astype(BF)
        o_ref[..., LANES * j : LANES * j + LANES] = found.reshape(shape)


def cfar_only_kernel(p_ref, n_ref, o_ref):
    narrow = p_ref[...].astype(BF)
    for j in range(o_ref.shape[1] // LANES):
        noise = dot(narrow[:, LANES * j : LANES * (j + 3)], n_ref[...])
        own = p_ref[:, LANES * (j + 1) : LANES * (j + 2)]
        o_ref[:, LANES * j : LANES * j + LANES] = (own / (noise + NOISE_FLOOR)).astype(BF)


def place_kernel(x_ref, o_ref):
    count, _, width = x_ref.shape
    for s in range(count):
        o_ref[:, width * s : width * s + width] = x_ref[s].astype(F32)


def complex_rows(re, im):
    top = np.stack([re, -im], -1)
    low = np.stack([im, re], -1)
    return np.stack([top, low], 1).reshape(2 * re.shape[0], 2 * re.shape[1])


def shards_split(signal, steering, spectrum):
    beams, chans = steering.shape[1], steering.shape[2]
    _, chan_own, pulse_own, gates = signal.shape
    zs, xs, ys = (lax.axis_size(a) for a in ("chan", "pulse", "range"))
    beam_own = beams // zs
    part = pulse_own // ys
    full = gates * ys
    block = gates // zs
    m_count = full // LANES
    groups = beam_own * part // ROWS
    pulses = pulse_own * xs

    w_real, w_imag = steering[0], steering[1]
    weights = jnp.concatenate(
        [jnp.concatenate([w_real, -w_imag], 1), jnp.concatenate([w_imag, w_real], 1)], 0
    )
    dy, dz, gr, cp, it = grid_ids(ys, zs, groups, 2, ROWS)
    bp = gr * ROWS + it
    left = cp * beams + dz * beam_own + bp // part
    left_pulse = dy * part + bp % part
    sz, ci, ch, pi = grid_ids(zs, 2, chan_own, pulse_own)
    right = ci * chans + sz * chan_own + ch
    form = expand(left, left_pulse, weights, right, pi)

    ms = np.arange(m_count)
    angle = 2.0 * np.pi * (np.outer(ms, ms) % m_count) / m_count
    outer_f = jnp.asarray(complex_rows(np.cos(angle), -np.sin(angle)), BF)
    outer_i = jnp.asarray(complex_rows(np.cos(angle), np.sin(angle)), BF)
    mk, mc, mi = grid_ids(m_count, 2, ROWS)
    outer_f = expand(mk * 2 + mc, mi, outer_f, mk * 2 + mc, mi)
    outer_i = expand(mk * 2 + mc, mi, outer_i, mk * 2 + mc, mi)
    ls = np.arange(LANES)
    angle = 2.0 * np.pi * (np.outer(ls, ls) % LANES) / LANES
    co, si = np.cos(angle), np.sin(angle)
    inner_f = jnp.asarray(np.block([[co, -si], [si, co]]), BF)
    inner_i = jnp.asarray(np.block([[co, si], [-si, co]]), BF)
    angle = 2.0 * np.pi * np.outer(ms, ls) / full
    twiddle = jnp.asarray(np.stack([np.cos(angle), -np.sin(angle)]), F32)
    spread = (2, m_count, ROWS, LANES)
    twiddle = jnp.broadcast_to(twiddle[:, :, None, :], spread)
    response = jnp.swapaxes(spectrum.reshape(2, LANES, m_count), 1, 2) * (1.0 / full)
    response = jnp.broadcast_to(response[:, :, None, :], spread)

    samples = lax.all_to_all(signal, "chan", split_axis=3, concat_axis=0, tiled=True)
    samples = samples.reshape(zs * 2 * chan_own * pulse_own, block)
    rows = 2 * beam_own * part
    formed = call(
        form_kernel, jax.ShapeDtypeStruct((ys * zs * rows, block), BF), "form"
    )(form, samples).reshape(ys * zs, rows, block)
    formed = lax.all_to_all(formed, ("range", "chan"), split_axis=0, concat_axis=0, tiled=True)

    blocks = ys * xs
    own = full // blocks
    padded = own + 2 * LANES
    packed = call(
        functools.partial(range_kernel, blocks),
        jax.ShapeDtypeStruct((blocks, rows, padded), BF),
        "compress",
    )(formed, outer_f, outer_i, twiddle, inner_f, inner_i, response)
    columns = lax.all_to_all(packed, ("range", "pulse"), split_axis=0, concat_axis=0, tiled=True)

    src, dst = np.arange(3 * LANES)[:, None] - LANES, np.arange(LANES)[None, :]
    gap = np.abs(src - dst)
    window = jnp.asarray(((gap > GUARD) & (gap <= GUARD + TRAIN)) / (2.0 * TRAIN), BF)

    dr, di = doppler_table(pulses)
    out_shape = jax.ShapeDtypeStruct((pulses * beam_own, own), BF)
    if 2 * pulses * beam_own <= 1024:
        table = jnp.concatenate([jnp.concatenate([dr, -di], 1), jnp.concatenate([di, dr], 1)], 0)
        oc, oq, ob, of = grid_ids(2, xs, beam_own, pulse_own)
        sy, sx, gr, cp, it = grid_ids(ys, xs, groups, 2, ROWS)
        bp = gr * ROWS + it
        pulse = sx * pulse_own + sy * part + bp % part
        mix = expand(oc * pulses + oq * pulse_own + of, ob, table, cp * pulses + pulse, bp // part)
        found = call(cfar_kernel, out_shape, "cfar")(
            mix, columns.reshape(blocks * rows, padded), window
        )
    else:
        v = columns.reshape(ys, xs, groups, 2, ROWS // part, part, padded)
        v = jnp.transpose(v, (3, 2, 4, 1, 0, 5, 6)).reshape(2, beam_own, pulses, padded)

        def product(t, x):
            return jnp.einsum("fp,bpr->fbr", t, x, preferred_element_type=F32)

        re = product(dr, v[0]) - product(di, v[1])
        im = product(dr, v[1]) + product(di, v[0])
        power = (re * re + im * im).reshape(xs, pulse_own, beam_own, padded)
        power = jnp.swapaxes(power, 1, 2).reshape(pulses * beam_own, padded)
        found = call(cfar_only_kernel, out_shape, "cfar")(power, window)
    found = found.reshape(xs, beam_own * pulse_own, own)
    found = lax.all_to_all(found, "pulse", split_axis=0, concat_axis=0, tiled=True)
    out = call(
        place_kernel, jax.ShapeDtypeStruct((beam_own * pulse_own, gates), F32), "place"
    )(found)
    return out.reshape(beam_own, pulse_own, gates)


MESH = pl.DeviceIdType.MESH


def widen(left, right, table):
    n, m = table.shape
    r, c = left.shape[1], right.shape[1]
    pick_l = (left[0] == lax.broadcasted_iota(jnp.int32, (r, n), 1)).astype(F32).astype(BF)
    pick_r = (right[0] == lax.broadcasted_iota(jnp.int32, (m, c), 0)).astype(F32).astype(BF)
    wide = dot(dot(pick_l, table[...]).astype(BF), pick_r)
    return jnp.where(left[1] == right[1], wide, 0.0).astype(BF)


def chain_kernel(
    sizes, sig, w_l, w_r, w_t, f_l, f_r, f_t, fi_t, tw, inf, ini, resp, d_l, d_r, d_t, win, out,
    recv1, send2, recv2, send3, recv3, send4, recv4, wide_w, wide_f, wide_i, wide_d, spread,
    acc, own_sem, s1, r1, s2, r2, s3, r3, s4, r4,
):
    zs, ys, xs = sizes
    block = recv1.shape[2]
    z, y, x = (lax.axis_index(a) for a in ("chan", "range", "pulse"))

    def zy(i):
        return {"range": lax.div(i, zs), "chan": lax.rem(i, zs)}

    def xy(i):
        return {"range": lax.div(i, xs), "pulse": lax.rem(i, xs)}

    n2, n3 = ys * zs, ys * xs
    me2, me3 = y * zs + z, y * xs + x
    barrier = pltpu.get_barrier_semaphore()
    peers = 0
    for k in range(1, n2):
        pl.semaphore_signal(
            barrier, inc=1, device_id=zy(lax.rem(me2 + k, n2)), device_id_type=MESH
        )
        peers += 1
    for dy in range(ys):
        for dx in range(1, xs):
            target = {"range": lax.rem(y + dy, ys), "pulse": lax.rem(x + dx, xs)}
            pl.semaphore_signal(barrier, inc=1, device_id=target, device_id_type=MESH)
            peers += 1
    pl.semaphore_wait(barrier, peers)

    def piece(i):
        return sig.at[:, pl.ds(pl.multiple_of(i * block, block), block)]

    def push(src, dst, send, recv, k, target):
        copy = pltpu.make_async_remote_copy(
            src_ref=src, dst_ref=dst, send_sem=send.at[k], recv_sem=recv.at[k],
            device_id=target, device_id_type=MESH,
        )
        copy.start()
        return copy

    first = []
    for k in range(1, zs):
        to = lax.rem(z + k, zs)
        first.append(push(piece(to), recv1.at[z], s1, r1, k, {"chan": to}))
    mine = pltpu.make_async_copy(piece(z), recv1.at[z], own_sem)
    mine.start()

    for s in range(zs):
        wide_w[s] = widen(w_l, w_r[s], w_t)
    wide_f[...] = widen(f_l, f_r, f_t)
    wide_i[...] = widen(f_l, f_r, fi_t)
    wide_d[...] = widen(d_l, d_r, d_t)
    m_count = tw.shape[1]
    for i in range(2):
        spread[i] = jnp.broadcast_to(tw[i][:, None, :], (m_count, ROWS, LANES))
        spread[2 + i] = jnp.broadcast_to(resp[i][:, None, :], (m_count, ROWS, LANES))

    mine.wait()
    acc[...] = dot(wide_w[z], recv1[z])
    for k in range(1, zs):
        src = lax.rem(z + zs - k, zs)
        first[k - 1].wait_recv()
        acc[...] += dot(wide_w[src], recv1[src])
    send2[...] = acc[...].astype(BF).reshape(send2.shape)
    second = []
    for k in range(1, n2):
        to = lax.rem(me2 + k, n2)
        second.append(push(send2.at[to], recv2.at[me2], s2, r2, k, zy(to)))
    recv2[me2] = send2[me2]
    for copy in second:
        copy.wait_recv()

    range_kernel(
        n3, recv2, wide_f, wide_i, spread.at[pl.ds(0, 2)], inf, ini, spread.at[pl.ds(2, 2)], send3
    )
    third = []
    for k in range(1, n3):
        to = lax.rem(me3 + k, n3)
        third.append(push(send3.at[to], recv3.at[me3], s3, r3, k, xy(to)))
    recv3[me3] = send3[me3]
    for copy in third:
        copy.wait_recv()

    cfar_kernel(wide_d, recv3, win, send4)
    fourth = []
    for k in range(1, xs):
        to = lax.rem(x + k, xs)
        fourth.append(push(send4.at[to], recv4.at[x], s4, r4, k, {"pulse": to}))
    recv4[x] = send4[x]
    for copy in fourth:
        copy.wait_recv()
    place_kernel(recv4, out)
    for copy in first + second + third + fourth:
        copy.wait_send()


def ids_pair(ids, tags):
    return np.stack([ids, tags]).astype(np.int32)


def shards_chain(signal, steering, spectrum):
    beams, chans = steering.shape[1], steering.shape[2]
    _, chan_own, pulse_own, gates = signal.shape
    zs, xs, ys = (lax.axis_size(a) for a in ("chan", "pulse", "range"))
    beam_own = beams // zs
    part = pulse_own // ys
    full = gates * ys
    block = gates // zs
    m_count = full // LANES
    groups = beam_own * part // ROWS
    pulses = pulse_own * xs
    rows = 2 * beam_own * part
    blocks = ys * xs
    own = full // blocks
    padded = own + 2 * LANES

    w_real, w_imag = steering[0], steering[1]
    weights = jnp.concatenate(
        [jnp.concatenate([w_real, -w_imag], 1), jnp.concatenate([w_imag, w_real], 1)], 0
    )
    dy, dz, gr, cp, it = grid_ids(ys, zs, groups, 2, ROWS)
    bp = gr * ROWS + it
    w_l = ids_pair(cp * beams + dz * beam_own + bp // part, dy * part + bp % part)[:, :, None]
    w_r = []
    for s in range(zs):
        ci, ch, pi = grid_ids(2, chan_own, pulse_own)
        w_r.append(ids_pair(ci * chans + s * chan_own + ch, pi)[:, None, :])
    w_r = np.stack(w_r)

    ms = np.arange(m_count)
    angle = 2.0 * np.pi * (np.outer(ms, ms) % m_count) / m_count
    outer_f = jnp.asarray(complex_rows(np.cos(angle), -np.sin(angle)), BF)
    outer_i = jnp.asarray(complex_rows(np.cos(angle), np.sin(angle)), BF)
    mk, mc, mi = grid_ids(m_count, 2, ROWS)
    f_ids = ids_pair(mk * 2 + mc, mi)
    ls = np.arange(LANES)
    angle = 2.0 * np.pi * (np.outer(ls, ls) % LANES) / LANES
    co, si = np.cos(angle), np.sin(angle)
    inner_f = jnp.asarray(np.block([[co, -si], [si, co]]), BF)
    inner_i = jnp.asarray(np.block([[co, si], [-si, co]]), BF)
    angle = 2.0 * np.pi * np.outer(ms, ls) / full
    twiddle = jnp.asarray(np.stack([np.cos(angle), -np.sin(angle)]), F32)
    response = jnp.swapaxes(spectrum.reshape(2, LANES, m_count), 1, 2) * (1.0 / full)

    src, dst = np.arange(3 * LANES)[:, None] - LANES, np.arange(LANES)[None, :]
    gap = np.abs(src - dst)
    window = jnp.asarray(((gap > GUARD) & (gap <= GUARD + TRAIN)) / (2.0 * TRAIN), BF)
    dr, di = doppler_table(pulses)
    table = jnp.concatenate([jnp.concatenate([dr, -di], 1), jnp.concatenate([di, dr], 1)], 0)
    oc, oq, ob, of = grid_ids(2, xs, beam_own, pulse_own)
    sy, sx, gr, cp, it = grid_ids(ys, xs, groups, 2, ROWS)
    bp = gr * ROWS + it
    pulse = sx * pulse_own + sy * part + bp % part
    d_l = ids_pair(oc * pulses + oq * pulse_own + of, ob)[:, :, None]
    d_r = ids_pair(cp * pulses + pulse, bp // part)[:, None, :]

    depth = 2 * chan_own * pulse_own
    kernel_rows = 2 * beams * pulse_own
    cells = beam_own * pulse_own
    vmem = pl.BlockSpec(memory_space=pltpu.VMEM)
    dma = pltpu.SemaphoreType.DMA
    out = pl.pallas_call(
        functools.partial(chain_kernel, (zs, ys, xs)),
        out_shape=jax.ShapeDtypeStruct((cells, gates), F32),
        in_specs=[pl.BlockSpec(memory_space=pl.ANY)] + [vmem] * 15,
        out_specs=vmem,
        scratch_shapes=[
            pltpu.VMEM((zs, depth, block), BF),
            pltpu.VMEM((ys * zs, rows, block), BF),
            pltpu.VMEM((ys * zs, rows, block), BF),
            pltpu.VMEM((blocks, rows, padded), BF),
            pltpu.VMEM((blocks, rows, padded), BF),
            pltpu.VMEM((xs, cells, own), BF),
            pltpu.VMEM((xs, cells, own), BF),
            pltpu.VMEM((zs, kernel_rows, depth), BF),
            pltpu.VMEM((m_count * 16, m_count * 16), BF),
            pltpu.VMEM((m_count * 16, m_count * 16), BF),
            pltpu.VMEM((2 * pulses * beam_own, blocks * rows), BF),
            pltpu.VMEM((4, m_count, ROWS, LANES), F32),
            pltpu.VMEM((kernel_rows, block), F32),
            dma,
            dma((zs,)), dma((zs,)),
            dma((ys * zs,)), dma((ys * zs,)),
            dma((blocks,)), dma((blocks,)),
            dma((xs,)), dma((xs,)),
        ],
        compiler_params=pltpu.CompilerParams(
            collective_id=0, has_side_effects=True, vmem_limit_bytes=VM
        ),
        name="chain",
    )(
        signal.reshape(depth, gates), w_l, w_r, weights,
        f_ids[:, :, None], f_ids[:, None, :], outer_f, outer_i,
        twiddle, inner_f, inner_i, response, d_l, d_r, table, window,
    )
    return out.reshape(beam_own, pulse_own, gates)


def shards(signal, steering, spectrum):
    pulses = signal.shape[2] * lax.axis_size("pulse")
    beam_own = steering.shape[1] // lax.axis_size("chan")
    small = 2 * pulses * beam_own <= 1024
    return (shards_chain if small else shards_split)(signal, steering, spectrum)


def solution(mesh):
    in_specs = (P(None, "chan", "pulse", "range"), P(), P())
    out_specs = P("chan", "pulse", "range")
    return jax.shard_map(shards, mesh=mesh, in_specs=in_specs, out_specs=out_specs, check_vma=False)
```

```python
import functools
import math

import jax
import jax.numpy as jnp
import numpy as np
from jax import lax
from jax.experimental import pallas as pl
from jax.experimental.pallas import tpu as pltpu
from jax.sharding import PartitionSpec as P

GUARD = 4
TRAIN = 16
NOISE_FLOOR = 0.25
LANES = 128
ROWS = 8
CHUNKS = 8
BF = jnp.bfloat16
F32 = jnp.float32
VM = 60 * 1024 * 1024


def dot(a, b):
    return jnp.dot(a, b, preferred_element_type=F32)


def doppler_table(count):
    ids = np.arange(count)
    angle = (np.outer(ids, ids) % count) * (2.0 * np.pi / count)
    scale = 1.0 / math.sqrt(count)
    return jnp.asarray(np.cos(angle) * scale, BF), jnp.asarray(-np.sin(angle) * scale, BF)


def expand(left_ids, left_tag, table, right_ids, right_tag):
    n, m = table.shape
    left = (jnp.asarray(left_ids, jnp.int32)[:, None] == jnp.arange(n)[None, :]).astype(BF)
    right = (jnp.arange(m)[:, None] == jnp.asarray(right_ids, jnp.int32)[None, :]).astype(BF)
    wide = dot(dot(left, table).astype(BF), right)
    same = jnp.asarray(left_tag, jnp.int32)[:, None] == jnp.asarray(right_tag, jnp.int32)[None, :]
    return jnp.where(same, wide, 0.0).astype(BF)


def grid_ids(*sizes):
    return [g.reshape(-1) for g in np.meshgrid(*[np.arange(s) for s in sizes], indexing="ij")]


def call(body, out_shape, name):
    return pl.pallas_call(
        body,
        out_shape=out_shape,
        compiler_params=pltpu.CompilerParams(vmem_limit_bytes=VM),
        name=name,
    )


def form_kernel(w_ref, x_ref, o_ref):
    o_ref[...] = dot(w_ref[...], x_ref[...]).astype(BF)


def range_kernel(blocks, x_ref, f_ref, fi_ref, t_ref, l_ref, li_ref, h_ref, o_ref):
    sources, rows, width = x_ref.shape
    per = width // LANES
    groups = rows // 16
    m_count = sources * per
    tile = []
    for g in range(groups):
        parts = [
            x_ref[s, 16 * g : 16 * g + 16, LANES * j : LANES * j + LANES]
            for s in range(sources)
            for j in range(per)
        ]
        tile.append(jnp.concatenate(parts, axis=0))
    outer = dot(f_ref[...], jnp.concatenate(tile, axis=1))
    tr, ti = t_ref[0], t_ref[1]
    hr, hi = h_ref[0], h_ref[1]
    back = []
    for g in range(groups):
        a = outer[:, LANES * g : LANES * g + LANES].reshape(m_count, 2, ROWS, LANES)
        ar, ai = a[:, 0], a[:, 1]
        b = jnp.concatenate([ar * tr - ai * ti, ar * ti + ai * tr], axis=-1)
        c = dot(b.reshape(m_count * ROWS, 2 * LANES).astype(BF), l_ref[...])
        c = c.reshape(m_count, ROWS, 2 * LANES)
        cr, ci = c[..., :LANES], c[..., LANES:]
        d = jnp.concatenate([cr * hr - ci * hi, cr * hi + ci * hr], axis=-1)
        e = dot(d.reshape(m_count * ROWS, 2 * LANES).astype(BF), li_ref[...])
        e = e.reshape(m_count, ROWS, 2 * LANES)
        er, ei = e[..., :LANES], e[..., LANES:]
        f = jnp.stack([er * tr + ei * ti, ei * tr - er * ti], axis=1)
        back.append(f.reshape(m_count * 16, LANES).astype(BF))
    y = dot(fi_ref[...], jnp.concatenate(back, axis=1)).astype(BF)
    span = m_count // blocks
    for d in range(blocks):
        for j in range(-1, span + 1):
            m = d * span + j
            for g in range(groups):
                if 0 <= m < m_count:
                    v = y[16 * m : 16 * m + 16, LANES * g : LANES * g + LANES]
                else:
                    v = jnp.zeros((16, LANES), BF)
                o_ref[d, 16 * g : 16 * g + 16, LANES * (j + 1) : LANES * (j + 2)] = v


def cfar_kernel(d_ref, x_ref, n_ref, o_ref):
    half = d_ref.shape[0] // 2
    mix = dot(d_ref[...], x_ref[...].reshape(d_ref.shape[1], x_ref.shape[-1]))
    re, im = mix[:half], mix[half:]
    power = re * re + im * im
    narrow = power.astype(BF)
    shape = o_ref.shape[:-1] + (LANES,)
    for j in range(o_ref.shape[-1] // LANES):
        noise = dot(narrow[:, LANES * j : LANES * (j + 3)], n_ref[...])
        own = power[:, LANES * (j + 1) : LANES * (j + 2)]
        found = (own / (noise + NOISE_FLOOR)).astype(BF)
        o_ref[..., LANES * j : LANES * j + LANES] = found.reshape(shape)


def cfar_only_kernel(p_ref, n_ref, o_ref):
    narrow = p_ref[...].astype(BF)
    for j in range(o_ref.shape[1] // LANES):
        noise = dot(narrow[:, LANES * j : LANES * (j + 3)], n_ref[...])
        own = p_ref[:, LANES * (j + 1) : LANES * (j + 2)]
        o_ref[:, LANES * j : LANES * j + LANES] = (own / (noise + NOISE_FLOOR)).astype(BF)


def place_kernel(x_ref, o_ref):
    count, _, width = x_ref.shape
    for s in range(count):
        o_ref[:, width * s : width * s + width] = x_ref[s].astype(F32)


def complex_rows(re, im):
    top = np.stack([re, -im], -1)
    low = np.stack([im, re], -1)
    return np.stack([top, low], 1).reshape(2 * re.shape[0], 2 * re.shape[1])


def shards_split(signal, steering, spectrum):
    beams, chans = steering.shape[1], steering.shape[2]
    _, chan_own, pulse_own, gates = signal.shape
    zs, xs, ys = (lax.axis_size(a) for a in ("chan", "pulse", "range"))
    beam_own = beams // zs
    part = pulse_own // ys
    full = gates * ys
    block = gates // zs
    m_count = full // LANES
    groups = beam_own * part // ROWS
    pulses = pulse_own * xs

    w_real, w_imag = steering[0], steering[1]
    weights = jnp.concatenate(
        [jnp.concatenate([w_real, -w_imag], 1), jnp.concatenate([w_imag, w_real], 1)], 0
    )
    dy, dz, gr, cp, it = grid_ids(ys, zs, groups, 2, ROWS)
    bp = gr * ROWS + it
    left = cp * beams + dz * beam_own + bp // part
    left_pulse = dy * part + bp % part
    sz, ci, ch, pi = grid_ids(zs, 2, chan_own, pulse_own)
    right = ci * chans + sz * chan_own + ch
    form = expand(left, left_pulse, weights, right, pi)

    ms = np.arange(m_count)
    angle = 2.0 * np.pi * (np.outer(ms, ms) % m_count) / m_count
    outer_f = jnp.asarray(complex_rows(np.cos(angle), -np.sin(angle)), BF)
    outer_i = jnp.asarray(complex_rows(np.cos(angle), np.sin(angle)), BF)
    mk, mc, mi = grid_ids(m_count, 2, ROWS)
    outer_f = expand(mk * 2 + mc, mi, outer_f, mk * 2 + mc, mi)
    outer_i = expand(mk * 2 + mc, mi, outer_i, mk * 2 + mc, mi)
    ls = np.arange(LANES)
    angle = 2.0 * np.pi * (np.outer(ls, ls) % LANES) / LANES
    co, si = np.cos(angle), np.sin(angle)
    inner_f = jnp.asarray(np.block([[co, -si], [si, co]]), BF)
    inner_i = jnp.asarray(np.block([[co, si], [-si, co]]), BF)
    angle = 2.0 * np.pi * np.outer(ms, ls) / full
    twiddle = jnp.asarray(np.stack([np.cos(angle), -np.sin(angle)]), F32)
    spread = (2, m_count, ROWS, LANES)
    twiddle = jnp.broadcast_to(twiddle[:, :, None, :], spread)
    response = jnp.swapaxes(spectrum.reshape(2, LANES, m_count), 1, 2) * (1.0 / full)
    response = jnp.broadcast_to(response[:, :, None, :], spread)

    samples = lax.all_to_all(signal, "chan", split_axis=3, concat_axis=0, tiled=True)
    samples = samples.reshape(zs * 2 * chan_own * pulse_own, block)
    rows = 2 * beam_own * part
    formed = call(
        form_kernel, jax.ShapeDtypeStruct((ys * zs * rows, block), BF), "form"
    )(form, samples).reshape(ys * zs, rows, block)
    formed = lax.all_to_all(formed, ("range", "chan"), split_axis=0, concat_axis=0, tiled=True)

    blocks = ys * xs
    own = full // blocks
    padded = own + 2 * LANES
    packed = call(
        functools.partial(range_kernel, blocks),
        jax.ShapeDtypeStruct((blocks, rows, padded), BF),
        "compress",
    )(formed, outer_f, outer_i, twiddle, inner_f, inner_i, response)
    columns = lax.all_to_all(packed, ("range", "pulse"), split_axis=0, concat_axis=0, tiled=True)

    src, dst = np.arange(3 * LANES)[:, None] - LANES, np.arange(LANES)[None, :]
    gap = np.abs(src - dst)
    window = jnp.asarray(((gap > GUARD) & (gap <= GUARD + TRAIN)) / (2.0 * TRAIN), BF)

    dr, di = doppler_table(pulses)
    out_shape = jax.ShapeDtypeStruct((pulses * beam_own, own), BF)
    if 2 * pulses * beam_own <= 1024:
        table = jnp.concatenate([jnp.concatenate([dr, -di], 1), jnp.concatenate([di, dr], 1)], 0)
        oc, oq, ob, of = grid_ids(2, xs, beam_own, pulse_own)
        sy, sx, gr, cp, it = grid_ids(ys, xs, groups, 2, ROWS)
        bp = gr * ROWS + it
        pulse = sx * pulse_own + sy * part + bp % part
        mix = expand(oc * pulses + oq * pulse_own + of, ob, table, cp * pulses + pulse, bp // part)
        found = call(cfar_kernel, out_shape, "cfar")(
            mix, columns.reshape(blocks * rows, padded), window
        )
    else:
        v = columns.reshape(ys, xs, groups, 2, ROWS // part, part, padded)
        v = jnp.transpose(v, (3, 2, 4, 1, 0, 5, 6)).reshape(2, beam_own, pulses, padded)

        def product(t, x):
            return jnp.einsum("fp,bpr->fbr", t, x, preferred_element_type=F32)

        re = product(dr, v[0]) - product(di, v[1])
        im = product(dr, v[1]) + product(di, v[0])
        power = (re * re + im * im).reshape(xs, pulse_own, beam_own, padded)
        power = jnp.swapaxes(power, 1, 2).reshape(pulses * beam_own, padded)
        found = call(cfar_only_kernel, out_shape, "cfar")(power, window)
    found = found.reshape(xs, beam_own * pulse_own, own)
    found = lax.all_to_all(found, "pulse", split_axis=0, concat_axis=0, tiled=True)
    out = call(
        place_kernel, jax.ShapeDtypeStruct((beam_own * pulse_own, gates), F32), "place"
    )(found)
    return out.reshape(beam_own, pulse_own, gates)


MESH = pl.DeviceIdType.MESH


def widen(left, right, table):
    n, m = table.shape
    r, c = left.shape[1], right.shape[1]
    pick_l = (left[0] == lax.broadcasted_iota(jnp.int32, (r, n), 1)).astype(F32).astype(BF)
    pick_r = (right[0] == lax.broadcasted_iota(jnp.int32, (m, c), 0)).astype(F32).astype(BF)
    wide = dot(dot(pick_l, table[...]).astype(BF), pick_r)
    return jnp.where(left[1] == right[1], wide, 0.0).astype(BF)


def chain_kernel(
    sizes, sig, w_l, w_r, w_t, f_l, f_r, f_t, fi_t, tw, inf, ini, resp, d_l, d_r, d_t, win, out,
    recv1, own1, sendp, recvp, send2, recv2, send3, recv3, send4, recv4, wide_w, wide_f, wide_i,
    wide_d, spread, acc, own_sem, s1, r1, sp, rp, s2, r2, s3, r3, s4, r4,
):
    zs, ys, xs = sizes
    chunks, _, block = recv1.shape
    z, y, x = (lax.axis_index(a) for a in ("chan", "range", "pulse"))

    def zy(i):
        return {"range": lax.div(i, zs), "chan": lax.rem(i, zs)}

    def xy(i):
        return {"range": lax.div(i, xs), "pulse": lax.rem(i, xs)}

    n2, n3 = ys * zs, ys * xs
    me2, me3 = y * zs + z, y * xs + x
    barrier = pltpu.get_barrier_semaphore()
    peers = 0
    for k in range(1, n2):
        pl.semaphore_signal(
            barrier, inc=1, device_id=zy(lax.rem(me2 + k, n2)), device_id_type=MESH
        )
        peers += 1
    for dy in range(ys):
        for dx in range(1, xs):
            target = {"range": lax.rem(y + dy, ys), "pulse": lax.rem(x + dx, xs)}
            pl.semaphore_signal(barrier, inc=1, device_id=target, device_id_type=MESH)
            peers += 1
    pl.semaphore_wait(barrier, peers)

    def piece(i):
        return sig.at[:, pl.ds(pl.multiple_of(i * block, block), block)]

    def plan(src, dst, send, recv, target):
        return pltpu.make_async_remote_copy(
            src_ref=src, dst_ref=dst, send_sem=send, recv_sem=recv,
            device_id=target, device_id_type=MESH,
        )

    def push(src, dst, send, recv, k, target):
        copy = plan(src, dst, send.at[k], recv.at[k], target)
        copy.start()
        return copy

    half = lax.div(z, 2)
    hub, edge = 1 + half, 3 * half
    is_hub = z == hub
    is_edge = z == edge
    raw = [plan(piece(c), recv1.at[c], s1.at[c], r1.at[c], {"chan": hub}) for c in range(chunks)]
    mine = [pltpu.make_async_copy(piece(c), own1.at[c], own_sem.at[c]) for c in range(chunks)]

    @pl.when(is_edge)
    def _():
        for c in range(chunks):
            raw[c].start()

    @pl.when(is_hub)
    def _():
        for c in range(chunks):
            mine[c].start()
        wide_w[0] = widen(w_l, w_r.at[hub], w_t)
        wide_w[1] = widen(w_l, w_r.at[edge], w_t)

    wide_f[...] = widen(f_l, f_r, f_t)
    wide_i[...] = widen(f_l, f_r, fi_t)
    wide_d[...] = widen(d_l, d_r, d_t)
    m_count = tw.shape[1]
    for i in range(2):
        spread[i] = jnp.broadcast_to(tw[i][:, None, :], (m_count, ROWS, LANES))
        spread[2 + i] = jnp.broadcast_to(resp[i][:, None, :], (m_count, ROWS, LANES))

    other_y = [lax.rem(y + k, ys) for k in range(1, ys)]
    half_rows = sendp.shape[1]

    def swap(c):
        return plan(sendp.at[c], recvp.at[c], sp.at[c], rp.at[c], {"chan": 3 - hub})

    def hand(c, i, to_y, zz, to_z):
        k = i * chunks + c
        slot = y * chunks + c
        return plan(
            send2.at[c, to_y, zz], recv2.at[slot], s2.at[k], r2.at[slot],
            {"range": to_y, "chan": to_z},
        )

    def hands(c):
        found = [hand(c, 0, y, half, edge)]
        for i, to_y in enumerate(other_y):
            found.append(hand(c, 1 + 2 * i, to_y, half, edge))
            found.append(hand(c, 2 + 2 * i, to_y, 1 - half, hub))
        return found

    def arrived(src_y, c):
        slot = src_y * chunks + c
        plan(
            send2.at[c, y, 0], recv2.at[slot], s2.at[0], r2.at[slot],
            {"range": src_y, "chan": hub},
        ).wait_recv()

    @pl.when(is_hub)
    def _():
        near = pl.ds(pl.multiple_of(half * half_rows, half_rows), half_rows)
        far = pl.ds(pl.multiple_of((1 - half) * half_rows, half_rows), half_rows)

        def finish(c):
            swap(c).wait_recv()
            total = (acc[c] + recvp[c].astype(F32)).astype(BF)
            send2[c] = total.reshape(send2.shape[1:])
            for copy in hands(c):
                copy.start()
            recv2[y * chunks + c] = send2[c, y, 1 - half]

        for c in range(chunks):
            mine[c].wait()
            raw[c].wait_recv()
            a, b = own1[c], recv1[c]
            sendp[c] = (dot(wide_w[0, far], a) + dot(wide_w[1, far], b)).astype(BF)
            swap(c).start()
            acc[c] = dot(wide_w[0, near], a) + dot(wide_w[1, near], b)
            if c > 0:
                finish(c - 1)
        finish(chunks - 1)
        for c in range(chunks):
            for to_y in other_y:
                arrived(to_y, c)
            swap(c).wait_send()
            for copy in hands(c):
                copy.wait_send()

    @pl.when(is_edge)
    def _():
        for c in range(chunks):
            for src_y in [y] + other_y:
                arrived(src_y, c)
            raw[c].wait_send()

    range_kernel(
        n3, recv2, wide_f, wide_i, spread.at[pl.ds(0, 2)], inf, ini, spread.at[pl.ds(2, 2)], send3
    )
    third = []
    for k in range(1, n3):
        to = lax.rem(me3 + k, n3)
        third.append(push(send3.at[to], recv3.at[me3], s3, r3, k, xy(to)))
    recv3[me3] = send3[me3]
    for copy in third:
        copy.wait_recv()

    cfar_kernel(wide_d, recv3, win, send4)
    fourth = []
    for k in range(1, xs):
        to = lax.rem(x + k, xs)
        fourth.append(push(send4.at[to], recv4.at[x], s4, r4, k, {"pulse": to}))
    recv4[x] = send4[x]
    for copy in fourth:
        copy.wait_recv()
    place_kernel(recv4, out)
    for copy in third + fourth:
        copy.wait_send()


def ids_pair(ids, tags):
    return np.stack([ids, tags]).astype(np.int32)


def shards_chain(signal, steering, spectrum):
    beams, chans = steering.shape[1], steering.shape[2]
    _, chan_own, pulse_own, gates = signal.shape
    zs, xs, ys = (lax.axis_size(a) for a in ("chan", "pulse", "range"))
    beam_own = beams // zs
    part = pulse_own // ys
    full = gates * ys
    chunks = CHUNKS
    block = gates // chunks
    m_count = full // LANES
    groups = beam_own * part // ROWS
    pulses = pulse_own * xs
    rows = 2 * beam_own * part
    blocks = ys * xs
    own = full // blocks
    padded = own + 2 * LANES

    w_real, w_imag = steering[0], steering[1]
    weights = jnp.concatenate(
        [jnp.concatenate([w_real, -w_imag], 1), jnp.concatenate([w_imag, w_real], 1)], 0
    )
    dh, dy, dz, gr, cp, it = grid_ids(2, ys, 2, groups, 2, ROWS)
    dz = dz + 2 * dh
    bp = gr * ROWS + it
    w_l = ids_pair(cp * beams + dz * beam_own + bp // part, dy * part + bp % part)[:, :, None]
    w_r = []
    for s in range(zs):
        ci, ch, pi = grid_ids(2, chan_own, pulse_own)
        w_r.append(ids_pair(ci * chans + s * chan_own + ch, pi)[:, None, :])
    w_r = np.stack(w_r)

    ms = np.arange(m_count)
    angle = 2.0 * np.pi * (np.outer(ms, ms) % m_count) / m_count
    outer_f = jnp.asarray(complex_rows(np.cos(angle), -np.sin(angle)), BF)
    outer_i = jnp.asarray(complex_rows(np.cos(angle), np.sin(angle)), BF)
    mk, mc, mi = grid_ids(m_count, 2, ROWS)
    f_ids = ids_pair(mk * 2 + mc, mi)
    ls = np.arange(LANES)
    angle = 2.0 * np.pi * (np.outer(ls, ls) % LANES) / LANES
    co, si = np.cos(angle), np.sin(angle)
    inner_f = jnp.asarray(np.block([[co, -si], [si, co]]), BF)
    inner_i = jnp.asarray(np.block([[co, si], [-si, co]]), BF)
    angle = 2.0 * np.pi * np.outer(ms, ls) / full
    twiddle = jnp.asarray(np.stack([np.cos(angle), -np.sin(angle)]), F32)
    response = jnp.swapaxes(spectrum.reshape(2, LANES, m_count), 1, 2) * (1.0 / full)

    src, dst = np.arange(3 * LANES)[:, None] - LANES, np.arange(LANES)[None, :]
    gap = np.abs(src - dst)
    window = jnp.asarray(((gap > GUARD) & (gap <= GUARD + TRAIN)) / (2.0 * TRAIN), BF)
    dr, di = doppler_table(pulses)
    table = jnp.concatenate([jnp.concatenate([dr, -di], 1), jnp.concatenate([di, dr], 1)], 0)
    oc, oq, ob, of = grid_ids(2, xs, beam_own, pulse_own)
    sy, sx, gr, cp, it = grid_ids(ys, xs, groups, 2, ROWS)
    bp = gr * ROWS + it
    pulse = sx * pulse_own + sy * part + bp % part
    d_l = ids_pair(oc * pulses + oq * pulse_own + of, ob)[:, :, None]
    d_r = ids_pair(cp * pulses + pulse, bp // part)[:, None, :]

    depth = 2 * chan_own * pulse_own
    kernel_rows = 2 * beams * pulse_own
    cells = beam_own * pulse_own
    vmem = pl.BlockSpec(memory_space=pltpu.VMEM)
    dma = pltpu.SemaphoreType.DMA
    out = pl.pallas_call(
        functools.partial(chain_kernel, (zs, ys, xs)),
        out_shape=jax.ShapeDtypeStruct((cells, gates), F32),
        in_specs=[pl.BlockSpec(memory_space=pl.ANY)] + [vmem] * 15,
        out_specs=vmem,
        scratch_shapes=[
            pltpu.VMEM((chunks, depth, block), BF),
            pltpu.VMEM((chunks, depth, block), BF),
            pltpu.VMEM((chunks, kernel_rows // 2, block), BF),
            pltpu.VMEM((chunks, kernel_rows // 2, block), BF),
            pltpu.VMEM((chunks, ys, 2, rows, block), BF),
            pltpu.VMEM((ys * chunks, rows, block), BF),
            pltpu.VMEM((blocks, rows, padded), BF),
            pltpu.VMEM((blocks, rows, padded), BF),
            pltpu.VMEM((xs, cells, own), BF),
            pltpu.VMEM((xs, cells, own), BF),
            pltpu.VMEM((2, kernel_rows, depth), BF),
            pltpu.VMEM((m_count * 16, m_count * 16), BF),
            pltpu.VMEM((m_count * 16, m_count * 16), BF),
            pltpu.VMEM((2 * pulses * beam_own, blocks * rows), BF),
            pltpu.VMEM((4, m_count, ROWS, LANES), F32),
            pltpu.VMEM((chunks, kernel_rows // 2, block), F32),
            dma((chunks,)),
            dma((chunks,)), dma((chunks,)),
            dma((chunks,)), dma((chunks,)),
            dma(((2 * ys - 1) * chunks,)), dma((ys * chunks,)),
            dma((blocks,)), dma((blocks,)),
            dma((xs,)), dma((xs,)),
        ],
        compiler_params=pltpu.CompilerParams(
            collective_id=0, has_side_effects=True, vmem_limit_bytes=VM
        ),
        name="chain",
    )(
        signal.reshape(depth, gates), w_l, w_r, weights,
        f_ids[:, :, None], f_ids[:, None, :], outer_f, outer_i,
        twiddle, inner_f, inner_i, response, d_l, d_r, table, window,
    )
    return out.reshape(beam_own, pulse_own, gates)


def shards(signal, steering, spectrum):
    pulses = signal.shape[2] * lax.axis_size("pulse")
    beam_own = steering.shape[1] // lax.axis_size("chan")
    small = 2 * pulses * beam_own <= 1024 and lax.axis_size("chan") == 4
    return (shards_chain if small else shards_split)(signal, steering, spectrum)


def solution(mesh):
    in_specs = (P(None, "chan", "pulse", "range"), P(), P())
    out_specs = P("chan", "pulse", "range")
    return jax.shard_map(shards, mesh=mesh, in_specs=in_specs, out_specs=out_specs, check_vma=False)
```

```python
import functools
import math

import jax
import jax.numpy as jnp
import numpy as np
from jax import lax
from jax.experimental import pallas as pl
from jax.experimental.pallas import tpu as pltpu
from jax.sharding import PartitionSpec as P

GUARD = 4
TRAIN = 16
NOISE_FLOOR = 0.25
LANES = 128
ROWS = 8
CHUNKS = 8
HALVES = 2
BF = jnp.bfloat16
F32 = jnp.float32
VM = 60 * 1024 * 1024


def dot(a, b):
    return jnp.dot(a, b, preferred_element_type=F32)


def doppler_table(count):
    ids = np.arange(count)
    angle = (np.outer(ids, ids) % count) * (2.0 * np.pi / count)
    scale = 1.0 / math.sqrt(count)
    return jnp.asarray(np.cos(angle) * scale, BF), jnp.asarray(-np.sin(angle) * scale, BF)


def expand(left_ids, left_tag, table, right_ids, right_tag):
    n, m = table.shape
    left = (jnp.asarray(left_ids, jnp.int32)[:, None] == jnp.arange(n)[None, :]).astype(BF)
    right = (jnp.arange(m)[:, None] == jnp.asarray(right_ids, jnp.int32)[None, :]).astype(BF)
    wide = dot(dot(left, table).astype(BF), right)
    same = jnp.asarray(left_tag, jnp.int32)[:, None] == jnp.asarray(right_tag, jnp.int32)[None, :]
    return jnp.where(same, wide, 0.0).astype(BF)


def grid_ids(*sizes):
    return [g.reshape(-1) for g in np.meshgrid(*[np.arange(s) for s in sizes], indexing="ij")]


def call(body, out_shape, name):
    return pl.pallas_call(
        body,
        out_shape=out_shape,
        compiler_params=pltpu.CompilerParams(vmem_limit_bytes=VM),
        name=name,
    )


def form_kernel(w_ref, x_ref, o_ref):
    o_ref[...] = dot(w_ref[...], x_ref[...]).astype(BF)


def range_kernel(blocks, x_ref, f_ref, fi_ref, t_ref, l_ref, li_ref, h_ref, o_ref):
    sources, rows, width = x_ref.shape
    per = width // LANES
    groups = rows // 16
    m_count = sources * per
    tile = []
    for g in range(groups):
        parts = [
            x_ref[s, 16 * g : 16 * g + 16, LANES * j : LANES * j + LANES]
            for s in range(sources)
            for j in range(per)
        ]
        tile.append(jnp.concatenate(parts, axis=0))
    outer = dot(f_ref[...], jnp.concatenate(tile, axis=1))
    tr, ti = t_ref[0], t_ref[1]
    hr, hi = h_ref[0], h_ref[1]
    back = []
    for g in range(groups):
        a = outer[:, LANES * g : LANES * g + LANES].reshape(m_count, 2, ROWS, LANES)
        ar, ai = a[:, 0], a[:, 1]
        b = jnp.concatenate([ar * tr - ai * ti, ar * ti + ai * tr], axis=-1)
        c = dot(b.reshape(m_count * ROWS, 2 * LANES).astype(BF), l_ref[...])
        c = c.reshape(m_count, ROWS, 2 * LANES)
        cr, ci = c[..., :LANES], c[..., LANES:]
        d = jnp.concatenate([cr * hr - ci * hi, cr * hi + ci * hr], axis=-1)
        e = dot(d.reshape(m_count * ROWS, 2 * LANES).astype(BF), li_ref[...])
        e = e.reshape(m_count, ROWS, 2 * LANES)
        er, ei = e[..., :LANES], e[..., LANES:]
        f = jnp.stack([er * tr + ei * ti, ei * tr - er * ti], axis=1)
        back.append(f.reshape(m_count * 16, LANES).astype(BF))
    y = dot(fi_ref[...], jnp.concatenate(back, axis=1)).astype(BF)
    span = m_count // blocks
    for d in range(blocks):
        for j in range(-1, span + 1):
            m = d * span + j
            for g in range(groups):
                if 0 <= m < m_count:
                    v = y[16 * m : 16 * m + 16, LANES * g : LANES * g + LANES]
                else:
                    v = jnp.zeros((16, LANES), BF)
                o_ref[d, 16 * g : 16 * g + 16, LANES * (j + 1) : LANES * (j + 2)] = v


def cfar_kernel(d_ref, x_ref, n_ref, o_ref):
    half = d_ref.shape[0] // 2
    mix = dot(d_ref[...], x_ref[...].reshape(d_ref.shape[1], x_ref.shape[-1]))
    re, im = mix[:half], mix[half:]
    power = re * re + im * im
    narrow = power.astype(BF)
    shape = o_ref.shape[:-1] + (LANES,)
    for j in range(o_ref.shape[-1] // LANES):
        noise = dot(narrow[:, LANES * j : LANES * (j + 3)], n_ref[...])
        own = power[:, LANES * (j + 1) : LANES * (j + 2)]
        found = (own / (noise + NOISE_FLOOR)).astype(BF)
        o_ref[..., LANES * j : LANES * j + LANES] = found.reshape(shape)


def cfar_only_kernel(p_ref, n_ref, o_ref):
    narrow = p_ref[...].astype(BF)
    for j in range(o_ref.shape[1] // LANES):
        noise = dot(narrow[:, LANES * j : LANES * (j + 3)], n_ref[...])
        own = p_ref[:, LANES * (j + 1) : LANES * (j + 2)]
        o_ref[:, LANES * j : LANES * j + LANES] = (own / (noise + NOISE_FLOOR)).astype(BF)


def place_kernel(x_ref, o_ref):
    count, _, width = x_ref.shape
    for s in range(count):
        o_ref[:, width * s : width * s + width] = x_ref[s].astype(F32)


def complex_rows(re, im):
    top = np.stack([re, -im], -1)
    low = np.stack([im, re], -1)
    return np.stack([top, low], 1).reshape(2 * re.shape[0], 2 * re.shape[1])


def shards_split(signal, steering, spectrum):
    beams, chans = steering.shape[1], steering.shape[2]
    _, chan_own, pulse_own, gates = signal.shape
    zs, xs, ys = (lax.axis_size(a) for a in ("chan", "pulse", "range"))
    beam_own = beams // zs
    part = pulse_own // ys
    full = gates * ys
    block = gates // zs
    m_count = full // LANES
    groups = beam_own * part // ROWS
    pulses = pulse_own * xs

    w_real, w_imag = steering[0], steering[1]
    weights = jnp.concatenate(
        [jnp.concatenate([w_real, -w_imag], 1), jnp.concatenate([w_imag, w_real], 1)], 0
    )
    dy, dz, gr, cp, it = grid_ids(ys, zs, groups, 2, ROWS)
    bp = gr * ROWS + it
    left = cp * beams + dz * beam_own + bp // part
    left_pulse = dy * part + bp % part
    sz, ci, ch, pi = grid_ids(zs, 2, chan_own, pulse_own)
    right = ci * chans + sz * chan_own + ch
    form = expand(left, left_pulse, weights, right, pi)

    ms = np.arange(m_count)
    angle = 2.0 * np.pi * (np.outer(ms, ms) % m_count) / m_count
    outer_f = jnp.asarray(complex_rows(np.cos(angle), -np.sin(angle)), BF)
    outer_i = jnp.asarray(complex_rows(np.cos(angle), np.sin(angle)), BF)
    mk, mc, mi = grid_ids(m_count, 2, ROWS)
    outer_f = expand(mk * 2 + mc, mi, outer_f, mk * 2 + mc, mi)
    outer_i = expand(mk * 2 + mc, mi, outer_i, mk * 2 + mc, mi)
    ls = np.arange(LANES)
    angle = 2.0 * np.pi * (np.outer(ls, ls) % LANES) / LANES
    co, si = np.cos(angle), np.sin(angle)
    inner_f = jnp.asarray(np.block([[co, -si], [si, co]]), BF)
    inner_i = jnp.asarray(np.block([[co, si], [-si, co]]), BF)
    angle = 2.0 * np.pi * np.outer(ms, ls) / full
    twiddle = jnp.asarray(np.stack([np.cos(angle), -np.sin(angle)]), F32)
    spread = (2, m_count, ROWS, LANES)
    twiddle = jnp.broadcast_to(twiddle[:, :, None, :], spread)
    response = jnp.swapaxes(spectrum.reshape(2, LANES, m_count), 1, 2) * (1.0 / full)
    response = jnp.broadcast_to(response[:, :, None, :], spread)

    samples = lax.all_to_all(signal, "chan", split_axis=3, concat_axis=0, tiled=True)
    samples = samples.reshape(zs * 2 * chan_own * pulse_own, block)
    rows = 2 * beam_own * part
    formed = call(
        form_kernel, jax.ShapeDtypeStruct((ys * zs * rows, block), BF), "form"
    )(form, samples).reshape(ys * zs, rows, block)
    formed = lax.all_to_all(formed, ("range", "chan"), split_axis=0, concat_axis=0, tiled=True)

    blocks = ys * xs
    own = full // blocks
    padded = own + 2 * LANES
    packed = call(
        functools.partial(range_kernel, blocks),
        jax.ShapeDtypeStruct((blocks, rows, padded), BF),
        "compress",
    )(formed, outer_f, outer_i, twiddle, inner_f, inner_i, response)
    columns = lax.all_to_all(packed, ("range", "pulse"), split_axis=0, concat_axis=0, tiled=True)

    src, dst = np.arange(3 * LANES)[:, None] - LANES, np.arange(LANES)[None, :]
    gap = np.abs(src - dst)
    window = jnp.asarray(((gap > GUARD) & (gap <= GUARD + TRAIN)) / (2.0 * TRAIN), BF)

    dr, di = doppler_table(pulses)
    out_shape = jax.ShapeDtypeStruct((pulses * beam_own, own), BF)
    if 2 * pulses * beam_own <= 1024:
        table = jnp.concatenate([jnp.concatenate([dr, -di], 1), jnp.concatenate([di, dr], 1)], 0)
        oc, oq, ob, of = grid_ids(2, xs, beam_own, pulse_own)
        sy, sx, gr, cp, it = grid_ids(ys, xs, groups, 2, ROWS)
        bp = gr * ROWS + it
        pulse = sx * pulse_own + sy * part + bp % part
        mix = expand(oc * pulses + oq * pulse_own + of, ob, table, cp * pulses + pulse, bp // part)
        found = call(cfar_kernel, out_shape, "cfar")(
            mix, columns.reshape(blocks * rows, padded), window
        )
    else:
        v = columns.reshape(ys, xs, groups, 2, ROWS // part, part, padded)
        v = jnp.transpose(v, (3, 2, 4, 1, 0, 5, 6)).reshape(2, beam_own, pulses, padded)

        def product(t, x):
            return jnp.einsum("fp,bpr->fbr", t, x, preferred_element_type=F32)

        re = product(dr, v[0]) - product(di, v[1])
        im = product(dr, v[1]) + product(di, v[0])
        power = (re * re + im * im).reshape(xs, pulse_own, beam_own, padded)
        power = jnp.swapaxes(power, 1, 2).reshape(pulses * beam_own, padded)
        found = call(cfar_only_kernel, out_shape, "cfar")(power, window)
    found = found.reshape(xs, beam_own * pulse_own, own)
    found = lax.all_to_all(found, "pulse", split_axis=0, concat_axis=0, tiled=True)
    out = call(
        place_kernel, jax.ShapeDtypeStruct((beam_own * pulse_own, gates), F32), "place"
    )(found)
    return out.reshape(beam_own, pulse_own, gates)


MESH = pl.DeviceIdType.MESH


def widen(left, right, table):
    n, m = table.shape
    r, c = left.shape[1], right.shape[1]
    pick_l = (left[0] == lax.broadcasted_iota(jnp.int32, (r, n), 1)).astype(F32).astype(BF)
    pick_r = (right[0] == lax.broadcasted_iota(jnp.int32, (m, c), 0)).astype(F32).astype(BF)
    wide = dot(dot(pick_l, table[...]).astype(BF), pick_r)
    return jnp.where(left[1] == right[1], wide, 0.0).astype(BF)


def chain_kernel(
    sizes, sig, w_l, w_r, w_t, f_l, f_r, f_t, fi_t, tw, inf, ini, resp, d_l, d_r, d_t, win, out,
    recv1, own1, sendp, recvp, send2, recv2, send3, recv3, send4, recv4, wide_w, wide_f, wide_i,
    wide_d, spread, acc, own_sem, s1, r1, sp, rp, s2, r2, s3, r3, s4, r4,
):
    zs, ys, xs = sizes
    chunks, _, block = recv1.shape
    z, y, x = (lax.axis_index(a) for a in ("chan", "range", "pulse"))

    def zy(i):
        return {"range": lax.div(i, zs), "chan": lax.rem(i, zs)}

    def xy(i):
        return {"range": lax.div(i, xs), "pulse": lax.rem(i, xs)}

    n2, n3 = ys * zs, ys * xs
    me2, me3 = y * zs + z, y * xs + x
    barrier = pltpu.get_barrier_semaphore()
    peers = 0
    for k in range(1, n2):
        pl.semaphore_signal(
            barrier, inc=1, device_id=zy(lax.rem(me2 + k, n2)), device_id_type=MESH
        )
        peers += 1
    for dy in range(ys):
        for dx in range(1, xs):
            target = {"range": lax.rem(y + dy, ys), "pulse": lax.rem(x + dx, xs)}
            pl.semaphore_signal(barrier, inc=1, device_id=target, device_id_type=MESH)
            peers += 1
    pl.semaphore_wait(barrier, peers)

    def piece(i):
        return sig.at[:, pl.ds(pl.multiple_of(i * block, block), block)]

    def plan(src, dst, send, recv, target):
        return pltpu.make_async_remote_copy(
            src_ref=src, dst_ref=dst, send_sem=send, recv_sem=recv,
            device_id=target, device_id_type=MESH,
        )

    def push(src, dst, send, recv, k, target):
        copy = plan(src, dst, send.at[k], recv.at[k], target)
        copy.start()
        return copy

    half = lax.div(z, 2)
    hub, edge = 1 + half, 3 * half
    is_hub = z == hub
    is_edge = z == edge
    raw = [plan(piece(c), recv1.at[c], s1.at[c], r1.at[c], {"chan": hub}) for c in range(chunks)]
    mine = [pltpu.make_async_copy(piece(c), own1.at[c], own_sem.at[c]) for c in range(chunks)]

    @pl.when(is_edge)
    def _():
        for c in range(chunks):
            raw[c].start()

    @pl.when(is_hub)
    def _():
        for c in range(chunks):
            mine[c].start()
        wide_w[0] = widen(w_l, w_r.at[hub], w_t)
        wide_w[1] = widen(w_l, w_r.at[edge], w_t)

    wide_f[...] = widen(f_l, f_r, f_t)
    wide_i[...] = widen(f_l, f_r, fi_t)
    wide_d[...] = widen(d_l, d_r, d_t)
    m_count = tw.shape[1]
    for i in range(2):
        spread[i] = jnp.broadcast_to(tw[i][:, None, :], (m_count, ROWS, LANES))
        spread[2 + i] = jnp.broadcast_to(resp[i][:, None, :], (m_count, ROWS, LANES))

    other_y = [lax.rem(y + k, ys) for k in range(1, ys)]
    half_rows = sendp.shape[1]

    def swap(c):
        return plan(sendp.at[c], recvp.at[c], sp.at[c], rp.at[c], {"chan": 3 - hub})

    def hand(c, i, to_y, zz, to_z):
        k = i * chunks + c
        slot = y * chunks + c
        return plan(
            send2.at[c, to_y, zz], recv2.at[slot], s2.at[k], r2.at[slot],
            {"range": to_y, "chan": to_z},
        )

    def hands(c):
        found = [hand(c, 0, y, half, edge)]
        for i, to_y in enumerate(other_y):
            found.append(hand(c, 1 + 2 * i, to_y, half, edge))
            found.append(hand(c, 2 + 2 * i, to_y, 1 - half, hub))
        return found

    def arrived(src_y, c):
        slot = src_y * chunks + c
        plan(
            send2.at[c, y, 0], recv2.at[slot], s2.at[0], r2.at[slot],
            {"range": src_y, "chan": hub},
        ).wait_recv()

    @pl.when(is_hub)
    def _():
        near = pl.ds(pl.multiple_of(half * half_rows, half_rows), half_rows)
        far = pl.ds(pl.multiple_of((1 - half) * half_rows, half_rows), half_rows)

        def finish(c):
            swap(c).wait_recv()
            total = (acc[c] + recvp[c].astype(F32)).astype(BF)
            send2[c] = total.reshape(send2.shape[1:])
            for copy in hands(c):
                copy.start()
            recv2[y * chunks + c] = send2[c, y, 1 - half]

        for c in range(chunks):
            mine[c].wait()
            raw[c].wait_recv()
            a, b = own1[c], recv1[c]
            sendp[c] = (dot(wide_w[0, far], a) + dot(wide_w[1, far], b)).astype(BF)
            swap(c).start()
            acc[c] = dot(wide_w[0, near], a) + dot(wide_w[1, near], b)
            if c > 0:
                finish(c - 1)
        finish(chunks - 1)
        for c in range(chunks):
            for to_y in other_y:
                arrived(to_y, c)
            swap(c).wait_send()
            for copy in hands(c):
                copy.wait_send()

    @pl.when(is_edge)
    def _():
        for c in range(chunks):
            for src_y in [y] + other_y:
                arrived(src_y, c)
            raw[c].wait_send()

    third, fourth = [], []
    part_rows = send3.shape[2]
    for h in range(HALVES):
        range_kernel(
            n3, recv2.at[:, pl.ds(part_rows * h, part_rows)], wide_f, wide_i,
            spread.at[pl.ds(0, 2)], inf, ini, spread.at[pl.ds(2, 2)], send3.at[h],
        )
        for k in range(1, n3):
            to = lax.rem(me3 + k, n3)
            third.append(
                push(send3.at[h, to], recv3.at[h, me3], s3, r3, h * n3 + k, xy(to))
            )
        recv3[h, me3] = send3[h, me3]

    for h in range(HALVES):
        for copy in third[h * (n3 - 1) : (h + 1) * (n3 - 1)]:
            copy.wait_recv()
        cfar_kernel(wide_d, recv3.at[h], win, send4.at[h])
        for k in range(1, xs):
            to = lax.rem(x + k, xs)
            fourth.append(
                push(send4.at[h, to], recv4.at[h, x], s4, r4, h * xs + k, {"pulse": to})
            )
        recv4[h, x] = send4[h, x]

    out_rows = send4.shape[2]
    for h in range(HALVES):
        for copy in fourth[h * (xs - 1) : (h + 1) * (xs - 1)]:
            copy.wait_recv()
        place_kernel(recv4.at[h], out.at[pl.ds(out_rows * h, out_rows)])
    for copy in third + fourth:
        copy.wait_send()


def ids_pair(ids, tags):
    return np.stack([ids, tags]).astype(np.int32)


def shards_chain(signal, steering, spectrum):
    beams, chans = steering.shape[1], steering.shape[2]
    _, chan_own, pulse_own, gates = signal.shape
    zs, xs, ys = (lax.axis_size(a) for a in ("chan", "pulse", "range"))
    beam_own = beams // zs
    part = pulse_own // ys
    full = gates * ys
    chunks = CHUNKS
    block = gates // chunks
    m_count = full // LANES
    groups = beam_own * part // ROWS
    pulses = pulse_own * xs
    rows = 2 * beam_own * part
    blocks = ys * xs
    own = full // blocks
    padded = own + 2 * LANES

    w_real, w_imag = steering[0], steering[1]
    weights = jnp.concatenate(
        [jnp.concatenate([w_real, -w_imag], 1), jnp.concatenate([w_imag, w_real], 1)], 0
    )
    dh, dy, dz, gr, cp, it = grid_ids(2, ys, 2, groups, 2, ROWS)
    dz = dz + 2 * dh
    bp = gr * ROWS + it
    w_l = ids_pair(cp * beams + dz * beam_own + bp // part, dy * part + bp % part)[:, :, None]
    w_r = []
    for s in range(zs):
        ci, ch, pi = grid_ids(2, chan_own, pulse_own)
        w_r.append(ids_pair(ci * chans + s * chan_own + ch, pi)[:, None, :])
    w_r = np.stack(w_r)

    ms = np.arange(m_count)
    angle = 2.0 * np.pi * (np.outer(ms, ms) % m_count) / m_count
    outer_f = jnp.asarray(complex_rows(np.cos(angle), -np.sin(angle)), BF)
    outer_i = jnp.asarray(complex_rows(np.cos(angle), np.sin(angle)), BF)
    mk, mc, mi = grid_ids(m_count, 2, ROWS)
    f_ids = ids_pair(mk * 2 + mc, mi)
    ls = np.arange(LANES)
    angle = 2.0 * np.pi * (np.outer(ls, ls) % LANES) / LANES
    co, si = np.cos(angle), np.sin(angle)
    inner_f = jnp.asarray(np.block([[co, -si], [si, co]]), BF)
    inner_i = jnp.asarray(np.block([[co, si], [-si, co]]), BF)
    angle = 2.0 * np.pi * np.outer(ms, ls) / full
    twiddle = jnp.asarray(np.stack([np.cos(angle), -np.sin(angle)]), F32)
    response = jnp.swapaxes(spectrum.reshape(2, LANES, m_count), 1, 2) * (1.0 / full)

    src, dst = np.arange(3 * LANES)[:, None] - LANES, np.arange(LANES)[None, :]
    gap = np.abs(src - dst)
    window = jnp.asarray(((gap > GUARD) & (gap <= GUARD + TRAIN)) / (2.0 * TRAIN), BF)
    dr, di = doppler_table(pulses)
    table = jnp.concatenate([jnp.concatenate([dr, -di], 1), jnp.concatenate([di, dr], 1)], 0)
    oc, oq, ob, of = grid_ids(2, xs, beam_own // HALVES, pulse_own)
    sy, sx, gr, cp, it = grid_ids(ys, xs, groups // HALVES, 2, ROWS)
    bp = gr * ROWS + it
    pulse = sx * pulse_own + sy * part + bp % part
    d_l = ids_pair(oc * pulses + oq * pulse_own + of, ob)[:, :, None]
    d_r = ids_pair(cp * pulses + pulse, bp // part)[:, None, :]

    depth = 2 * chan_own * pulse_own
    kernel_rows = 2 * beams * pulse_own
    cells = beam_own * pulse_own
    vmem = pl.BlockSpec(memory_space=pltpu.VMEM)
    dma = pltpu.SemaphoreType.DMA
    out = pl.pallas_call(
        functools.partial(chain_kernel, (zs, ys, xs)),
        out_shape=jax.ShapeDtypeStruct((cells, gates), F32),
        in_specs=[pl.BlockSpec(memory_space=pl.ANY)] + [vmem] * 15,
        out_specs=vmem,
        scratch_shapes=[
            pltpu.VMEM((chunks, depth, block), BF),
            pltpu.VMEM((chunks, depth, block), BF),
            pltpu.VMEM((chunks, kernel_rows // 2, block), BF),
            pltpu.VMEM((chunks, kernel_rows // 2, block), BF),
            pltpu.VMEM((chunks, ys, 2, rows, block), BF),
            pltpu.VMEM((ys * chunks, rows, block), BF),
            pltpu.VMEM((HALVES, blocks, rows // HALVES, padded), BF),
            pltpu.VMEM((HALVES, blocks, rows // HALVES, padded), BF),
            pltpu.VMEM((HALVES, xs, cells // HALVES, own), BF),
            pltpu.VMEM((HALVES, xs, cells // HALVES, own), BF),
            pltpu.VMEM((2, kernel_rows, depth), BF),
            pltpu.VMEM((m_count * 16, m_count * 16), BF),
            pltpu.VMEM((m_count * 16, m_count * 16), BF),
            pltpu.VMEM((2 * pulses * beam_own // HALVES, blocks * rows // HALVES), BF),
            pltpu.VMEM((4, m_count, ROWS, LANES), F32),
            pltpu.VMEM((chunks, kernel_rows // 2, block), F32),
            dma((chunks,)),
            dma((chunks,)), dma((chunks,)),
            dma((chunks,)), dma((chunks,)),
            dma(((2 * ys - 1) * chunks,)), dma((ys * chunks,)),
            dma((HALVES * blocks,)), dma((HALVES * blocks,)),
            dma((HALVES * xs,)), dma((HALVES * xs,)),
        ],
        compiler_params=pltpu.CompilerParams(
            collective_id=0, has_side_effects=True, vmem_limit_bytes=VM
        ),
        name="chain",
    )(
        signal.reshape(depth, gates), w_l, w_r, weights,
        f_ids[:, :, None], f_ids[:, None, :], outer_f, outer_i,
        twiddle, inner_f, inner_i, response, d_l, d_r, table, window,
    )
    return out.reshape(beam_own, pulse_own, gates)


def shards(signal, steering, spectrum):
    pulses = signal.shape[2] * lax.axis_size("pulse")
    beam_own = steering.shape[1] // lax.axis_size("chan")
    small = 2 * pulses * beam_own <= 1024 and lax.axis_size("chan") == 4
    return (shards_chain if small else shards_split)(signal, steering, spectrum)


def solution(mesh):
    in_specs = (P(None, "chan", "pulse", "range"), P(), P())
    out_specs = P("chan", "pulse", "range")
    return jax.shard_map(shards, mesh=mesh, in_specs=in_specs, out_specs=out_specs, check_vma=False)
```
